32 devices in a mesh: row: 2 (over y), col: 16 (over z, x, core).
Axes of the slice: x: 2, y: 2, z: 4, core: 2. Of those that a mesh axis runs over, the one named last changes fastest.
Arguments:
- previous: bfloat16 [4, 32, 128, 256], P(None, 'row', 'col'), may hold values from -6 to 6
- skip_coarse: bfloat16 [4, 32, 128, 256], P(None, 'row', 'col'), may hold values from -6 to 6
- skip_fine: bfloat16 [4, 64, 256, 256], P(None, 'row', 'col'), may hold values from -6 to 6
- coarse_convs: bfloat16 [4, 3, 3, 256, 256], replicated, may hold values from -0.125 to 0.125
- coarse_biases: float32 [4, 256], replicated, may hold values from -3 to 3
- coarse_project: bfloat16 [256, 256], replicated, may hold values from -0.375 to 0.375
- coarse_offset: float32 [256], replicated, may hold values from -3 to 3
- fine_convs: bfloat16 [4, 3, 3, 256, 256], replicated, may hold values from -0.125 to 0.125
- fine_biases: float32 [4, 256], replicated, may hold values from -3 to 3
- fine_project: bfloat16 [256, 256], replicated, may hold values from -0.375 to 0.375
- fine_offset: float32 [256], replicated, may hold values from -3 to 3
Outputs:
- decoded: bfloat16 [4, 128, 512, 256], P(None, 'row', 'col')
The draws below stay inside these ranges and needn't reach their ends.
All inputs are finite; a program needn't handle non-finite values.
Results may differ from the reference program's by a relative error of at most 0.012.
Values may be sent and summed in bfloat16 or wider, within the bound.
A program may use at most 128 MiB of HBM per device.

```python
import jax
import jax.numpy as jnp
from jax import lax

C = 256
B = 4
H8 = 32
W8 = 128


def level_of(key, shape, cuts, low, high):
    def one(axis_at, parts):
        draws = jax.random.uniform(jax.random.fold_in(jax.random.fold_in(key, 6), axis_at), (parts,), jnp.float32, low / len(cuts), high / len(cuts))
        return jnp.repeat(jnp.exp(draws), shape[axis_at] // parts).reshape((-1,) + (1,) * (len(shape) - axis_at - 1))

    loudness = one(*cuts[0])
    for cut in cuts[1:]:
        loudness = loudness * one(*cut)
    return loudness


def centred(key, shape, spread, most, shards=(), dtype=jnp.bfloat16):
    drawn = jax.random.normal(key, shape, jnp.float32) * spread
    if len(shards) > 0:
        drawn = level_of(key, shape, shards, -0.22, 0.18) * drawn
    return jnp.clip(drawn, min=-most, max=most).astype(dtype)


def setup_inputs(seed: int = 0) -> dict:
    key_list = jax.random.split(jax.random.key(seed), 12)
    return {
        "previous": centred(key_list[0], (B, H8, W8, C), 1.0, 6.0, ((1, 2), (2, 16))),
        "skip_coarse": centred(key_list[1], (B, H8, W8, C), 1.0, 6.0, ((1, 2), (2, 16))),
        "skip_fine": centred(key_list[2], (B, 2 * H8, 2 * W8, C), 1.0, 6.0, ((1, 2), (2, 16))),
        "coarse_convs": centred(key_list[3], (4, 3, 3, C, C), (9 * C) ** -0.5, 0.125),
        "coarse_biases": centred(key_list[4], (4, C), 0.5, 3.0, (), jnp.float32),
        "coarse_project": centred(key_list[5], (C, C), C ** -0.5, 0.375),
        "coarse_offset": centred(key_list[6], (C,), 0.5, 3.0, (), jnp.float32),
        "fine_convs": centred(key_list[7], (4, 3, 3, C, C), (9 * C) ** -0.5, 0.125),
        "fine_biases": centred(key_list[8], (4, C), 0.5, 3.0, (), jnp.float32),
        "fine_project": centred(key_list[9], (C, C), C ** -0.5, 0.375),
        "fine_offset": centred(key_list[10], (C,), 0.5, 3.0, (), jnp.float32),
    }


def convolve(image, kernel, bias):
    padded = jnp.pad(image, ((0, 0), (1, 1), (1, 1), (0, 0)))
    result = lax.conv_general_dilated(padded, kernel, (1, 1), "VALID", dimension_numbers=("NHWC", "HWIO", "NHWC"), preferred_element_type=jnp.float32)
    return result + bias


def residual_unit(inputs, kernels, biases, first):
    active = jax.nn.relu(inputs).astype(jnp.bfloat16)
    hidden = jax.nn.relu(convolve(active, kernels[first], biases[first])).astype(jnp.bfloat16)
    return inputs.astype(jnp.float32) + convolve(hidden, kernels[first + 1], biases[first + 1])


def double_axis(values, axis):
    count = values.shape[axis]
    padded = jnp.concatenate([lax.slice_in_dim(values, 0, 1, axis=axis), values, lax.slice_in_dim(values, count - 1, count, axis=axis)], axis=axis)
    before = lax.slice_in_dim(padded, 0, count, axis=axis)
    after = lax.slice_in_dim(padded, 2, count + 2, axis=axis)
    even = 0.75 * values + 0.25 * before
    odd = 0.75 * values + 0.25 * after
    stacked = jnp.stack([even, odd], axis=axis + 1)
    shape = list(values.shape)
    shape[axis] = 2 * count
    return stacked.reshape(shape)


def upsample(image):
    values = image.astype(jnp.float32)
    return double_axis(double_axis(values, 1), 2).astype(jnp.bfloat16)


def reference(previous, skip_coarse, skip_fine, coarse_convs, coarse_biases, coarse_project, coarse_offset, fine_convs, fine_biases, fine_project, fine_offset):
    sum_coarse = previous.astype(jnp.float32) + residual_unit(skip_coarse, coarse_convs, coarse_biases, 0)
    top_coarse = residual_unit(sum_coarse, coarse_convs, coarse_biases, 2).astype(jnp.bfloat16)
    joined_coarse = (jnp.dot(upsample(top_coarse), coarse_project, preferred_element_type=jnp.float32) + coarse_offset).astype(jnp.bfloat16)
    sum_fine = joined_coarse.astype(jnp.float32) + residual_unit(skip_fine, fine_convs, fine_biases, 0)
    top_fine = residual_unit(sum_fine, fine_convs, fine_biases, 2).astype(jnp.bfloat16)
    return (jnp.dot(upsample(top_fine), fine_project, preferred_element_type=jnp.float32) + fine_offset).astype(jnp.bfloat16)
```

```python
import functools

import jax
import jax.numpy as jnp
import numpy as np
from jax import lax
from jax.experimental import pallas as pl
from jax.experimental.pallas import tpu as pltpu
from jax.sharding import PartitionSpec as P

SUB = 16
BF = jnp.bfloat16
F32 = jnp.float32
DIRECTIONS = ((0, -1), (0, 1), (-1, 0), (1, 0), (-1, -1), (-1, 1), (1, -1), (1, 1))


def roll(value, shift):
    shift = shift % SUB
    if shift == 0:
        return value
    axis = value.ndim - 2
    if value.ndim == 3:
        return jnp.concatenate([value[:, SUB - shift :], value[:, : SUB - shift]], axis=1)
    return jnp.concatenate([value[SUB - shift :], value[: SUB - shift]], axis=axis)


class Level:
    def __init__(self, images, stage, packed, landed, corners, send, recv):
        self.image = images.at[stage]
        self.packed = packed.at[stage]
        self.landed = landed.at[stage]
        self.corners = corners.at[stage]
        self.send = send.at[stage]
        self.recv = recv.at[stage]
        self.rows = images.shape[1] - 2
        self.cols = images.shape[2] - 2


class Place:
    def __init__(self):
        self.row = lax.axis_index("row")
        self.col = lax.axis_index("col")
        self.rows = lax.axis_size("row")
        self.cols = lax.axis_size("col")

    def has(self, dr, dc):
        ok = None
        tests = []
        if dr == -1:
            tests.append(self.row > 0)
        if dr == 1:
            tests.append(self.row < self.rows - 1)
        if dc == -1:
            tests.append(self.col > 0)
        if dc == 1:
            tests.append(self.col < self.cols - 1)
        for test in tests:
            ok = test if ok is None else jnp.logical_and(ok, test)
        return ok

    def peers(self):
        def around(index, count):
            return 1 + (index > 0).astype(jnp.int32) + (index < count - 1).astype(jnp.int32)

        return around(self.row, self.rows) * around(self.col, self.cols) - 1

    def at(self, dr, dc):
        return (self.row + dr, self.col + dc)


def sub_index(shape):
    return lax.broadcasted_iota(jnp.int32, shape, len(shape) - 2)


def copies(place, lv):
    r, c = lv.rows, lv.cols
    im = lv.image
    ends = (
        (im.at[1 : r + 1, 1], im.at[1 : r + 1, c + 1]),
        (im.at[1 : r + 1, c], im.at[1 : r + 1, 0]),
        (lv.packed.at[0], lv.landed.at[1]),
        (lv.packed.at[1], lv.landed.at[0]),
        (im.at[1, 1], lv.corners.at[3]),
        (im.at[1, c], lv.corners.at[2]),
        (im.at[r, 1], lv.corners.at[1]),
        (im.at[r, c], lv.corners.at[0]),
    )
    return [
        pltpu.make_async_remote_copy(
            src_ref=src,
            dst_ref=dst,
            send_sem=lv.send.at[i],
            recv_sem=lv.recv.at[i],
            device_id=place.at(*DIRECTIONS[i]),
            device_id_type=pl.DeviceIdType.MESH,
        )
        for i, (src, dst) in enumerate(ends)
    ]


def exchange(place, lv, batch):
    r, c = lv.rows, lv.cols
    groups = SUB // batch
    channels = lv.image.shape[-1]
    moves = copies(place, lv)
    for i in (0, 1):
        pl.when(place.has(*DIRECTIONS[i]))(moves[i].start)
    slot = sub_index((c // groups, SUB, channels)) // batch
    for side, row in ((0, 1), (1, r)):
        v = lv.image[row, 1 : c + 1].astype(F32).reshape(c // groups, groups, SUB, channels)
        total = None
        for q in range(groups):
            part = roll(v[:, q], batch * (q if side == 0 else q + 1))
            total = part if total is None else jnp.where(slot == q, part, total)
        lv.packed[side] = total.astype(BF)
    for i in range(2, 8):
        pl.when(place.has(*DIRECTIONS[i]))(moves[i].start)


def settle(place, lv, batch, replicate):
    r, c = lv.rows, lv.cols
    im, landed, corners = lv.image, lv.landed, lv.corners
    groups = SUB // batch
    channels = im.shape[-1]
    moves = copies(place, lv)
    for i, (dr, dc) in enumerate(DIRECTIONS):
        pl.when(place.has(dr, dc))(moves[i].wait_send)
        pl.when(place.has(-dr, -dc))(moves[i].wait_recv)

    no_up = place.row == 0
    no_down = place.row == place.rows - 1
    no_left = place.col == 0
    no_right = place.col == place.cols - 1

    def rolled(tile, shift):
        return roll(tile.astype(F32), shift).astype(BF)

    for missing, at, edge in ((no_left, 0, 1), (no_right, c + 1, c)):

        @pl.when(missing)
        def _(at=at, edge=edge):
            if replicate:
                im[1 : r + 1, at] = im[1 : r + 1, edge]
            else:
                im[1 : r + 1, at] = jnp.zeros((r, SUB, channels), BF)

    for side, missing in ((0, no_up), (1, no_down)):

        @pl.when(missing)
        def _(side=side):
            if replicate:
                landed[side] = lv.packed[side]
            else:
                landed[side] = jnp.zeros((c // groups, SUB, channels), BF)

    last = c // groups - 1
    for k, vertical, horizontal in (
        (0, no_up, no_left),
        (1, no_up, no_right),
        (2, no_down, no_left),
        (3, no_down, no_right),
    ):
        if not replicate:

            @pl.when(jnp.logical_or(vertical, horizontal))
            def _(k=k):
                corners[k] = jnp.zeros((SUB, channels), BF)

        else:
            side = k // 2
            turn = -batch if side == 0 else batch
            row = 1 if side == 0 else r
            col = 0 if k % 2 == 0 else c + 1

            @pl.when(vertical)
            def _(k=k, turn=turn, row=row, col=col):
                corners[k] = rolled(im[row, col], turn)

            shift = (-batch, 0, 0, batch)[k]
            block = 0 if k % 2 == 0 else last

            @pl.when(jnp.logical_and(jnp.logical_not(vertical), horizontal))
            def _(k=k, side=side, shift=shift, block=block):
                corners[k] = rolled(landed[side, block], shift)

    group = sub_index((c + 2, SUB, channels)) // batch
    for side in (0, 1):
        near = roll(im[r if side == 0 else 1].astype(F32), batch if side == 0 else -batch)
        wide = landed[side].astype(F32)
        parts = [
            roll(wide, -batch * q if side == 0 else batch * (groups - 1 - q))
            for q in range(groups)
        ]
        inner = jnp.stack(parts, axis=1).reshape(c, SUB, channels)
        turn = batch if side == 0 else -batch
        ends = [
            roll(corners[2 * side + k].astype(F32), turn).reshape(1, SUB, channels) for k in (0, 1)
        ]
        outer = jnp.concatenate([ends[0], inner, ends[1]], axis=0)
        chosen = 0 if side == 0 else groups - 1
        im[0 if side == 0 else r + 1] = jnp.where(group == chosen, outer, near).astype(BF)


def conv_rows(lv, weight, start, count):
    c = lv.cols
    channels = lv.image.shape[-1]
    taps = [
        lv.image[pl.ds(start + dr, count), dc : dc + c].reshape(count * c * SUB, channels)
        for dr in range(3)
        for dc in range(3)
    ]
    return jnp.dot(jnp.concatenate(taps, axis=1), weight[...], preferred_element_type=F32)


def body(
    batch,
    prev,
    skip_c,
    skip_f,
    cw_hbm,
    cb,
    cp,
    co,
    fw_hbm,
    fb,
    fp,
    perm_c,
    perm_f,
    out,
    ic,
    if_,
    pack_c,
    pack_f,
    land_c,
    land_f,
    corner_c,
    corner_f,
    cw,
    fw,
    xc,
    xf,
    sum_f,
    send_c,
    recv_c,
    send_f,
    recv_f,
    wsem,
):
    place = Place()
    channels = skip_c.shape[-1]
    loads = {}
    for i in range(4):
        for k, (src, dst) in enumerate(((cw_hbm, cw), (fw_hbm, fw))):
            loads[k, i] = pltpu.make_async_copy(src.at[i], dst.at[i], wsem.at[k, i])
    for key in ((0, 0), (1, 0), (0, 1), (1, 1), (0, 2), (0, 3), (1, 2), (1, 3)):
        loads[key].start()

    barrier = pltpu.get_barrier_semaphore()
    for d in DIRECTIONS:

        @pl.when(place.has(*d))
        def _(d=d):
            pl.semaphore_signal(
                barrier, inc=1, device_id=place.at(*d), device_id_type=pl.DeviceIdType.MESH
            )

    lc = [Level(ic, s, pack_c, land_c, corner_c, send_c, recv_c) for s in range(5)]
    lf = [Level(if_, s, pack_f, land_f, corner_f, send_f, recv_f) for s in range(5)]
    rc, cc, rf, cf = lc[0].rows, lc[0].cols, lf[0].rows, lf[0].cols

    def regroup(ref, perm, row):
        tile = ref[:, :, row].reshape(perm.shape[0], channels)
        return jnp.dot(perm[...], tile, preferred_element_type=F32).reshape(-1, SUB, channels)

    @pl.loop(0, rc)
    def _(row):
        v = regroup(skip_c, perm_c, row)
        xc[row] = v + regroup(prev, perm_c, row)
        ic[0, row + 1, 1 : cc + 1] = jnp.maximum(v, 0.0).astype(BF)


    pl.semaphore_wait(barrier, place.peers())

    exchange(place, lc[0], batch)

    @pl.loop(0, rf)
    def _(row):
        v = regroup(skip_f, perm_f, row)
        xf[row] = v.astype(BF)
        if_[0, row + 1, 1 : cf + 1] = jnp.maximum(v, 0.0).astype(BF)

    exchange(place, lf[0], batch)

    def coarse(stage, finish):
        settle(place, lc[stage], batch, False)
        loads[0, stage].wait()
        v = conv_rows(lc[stage], cw.at[stage], 0, rc) + cb[stage : stage + 1]
        v = finish(v.reshape(rc, cc, SUB, channels))
        lc[stage + 1].image[1 : rc + 1, 1 : cc + 1] = v
        exchange(place, lc[stage + 1], batch)

    step = 2 if rf % 2 == 0 else 1

    def fine(stage, finish, first, last):
        @pl.loop(first, last)
        def _(i):
            v = conv_rows(lf[stage], fw.at[stage], i * step, step) + fb[stage : stage + 1]
            finish(i * step, v.reshape(step, cf, SUB, channels))

    def fine_ready(stage):
        settle(place, lf[stage], batch, False)
        loads[1, stage].wait()

    def hidden(v):
        return jnp.maximum(v, 0.0).astype(BF)

    def summed(v):
        v = v + xc[...]
        xc[...] = v
        return jnp.maximum(v, 0.0).astype(BF)

    def lifted(v):
        top = (v + xc[...]).astype(BF).reshape(rc * cc * SUB, channels)
        z = jnp.dot(top, cp[...], preferred_element_type=F32)
        return z.astype(BF).reshape(rc, cc, SUB, channels)

    def keep_hidden(stage):
        def finish(row, v):
            if_[stage + 1, pl.ds(row + 1, step), 1 : cf + 1] = hidden(v)

        return finish

    def keep_unit(row, v):
        sum_f[pl.ds(row, step)] = v + xf[pl.ds(row, step)].astype(F32)

    def keep_top(row, v):
        top = (v + sum_f[pl.ds(row, step)]).astype(BF).reshape(step * cf * SUB, channels)
        z = jnp.dot(top, fp[...], preferred_element_type=F32)
        if_[4, pl.ds(row + 1, step), 1 : cf + 1] = z.astype(BF).reshape(step, cf, SUB, channels)

    steps = rf // step
    half = steps // 2
    coarse(0, hidden)
    fine_ready(0)
    fine(0, keep_hidden(0), 0, steps)
    exchange(place, lf[1], batch)
    coarse(1, summed)
    fine_ready(1)
    fine(1, keep_unit, 0, half)
    coarse(2, hidden)
    fine(1, keep_unit, half, steps)
    coarse(3, lifted)
    settle(place, lc[4], batch, True)

    @pl.loop(0, rc)
    def _(row):
        mid = 0.75 * ic[4, row + 1].astype(F32)
        for p in range(2):
            v = mid + 0.25 * ic[4, row + 2 * p].astype(F32)
            core = 0.75 * v[1 : cc + 1]
            even = core + 0.25 * v[0:cc]
            odd = core + 0.25 * v[2 : cc + 2]
            both = jnp.stack([even, odd], axis=1).reshape(cf, SUB, channels)
            joined = (both + co[...]).astype(BF).astype(F32)
            total = joined + sum_f[2 * row + p]
            sum_f[2 * row + p] = total
            if_[2, 2 * row + p + 1, 1 : cf + 1] = jnp.maximum(total, 0.0).astype(BF)

    exchange(place, lf[2], batch)
    fine_ready(2)
    fine(2, keep_hidden(2), 0, steps)
    exchange(place, lf[3], batch)
    fine_ready(3)
    fine(3, keep_top, 0, steps)
    exchange(place, lf[4], batch)
    settle(place, lf[4], batch, True)

    @pl.loop(0, rf + 2)
    def _(row):
        out[row] = if_[4, row]


def raise_body(batch, z, spread, offset, out):
    row = pl.program_id(0)
    channels = z.shape[-1]
    mid = 0.75 * z[row + 1].astype(F32)
    for p in range(2):
        v = (mid + 0.25 * z[row + 2 * p].astype(F32)).astype(BF).reshape(-1, channels)
        res = jnp.dot(spread[...], v, preferred_element_type=F32) + offset[...]
        out[:, :, p] = res.astype(BF).reshape(batch, SUB // batch, -1, channels)


def regroup_matrix(batch, cols):
    groups = SUB // batch
    m = np.zeros((cols, groups, batch, batch, groups, cols), np.float32)
    for c in range(cols):
        for g in range(groups):
            for b in range(batch):
                m[c, g, b, b, g, c] = 1.0
    return jnp.asarray(m.reshape(cols * SUB, cols * SUB), BF)


def spread_matrix(batch, cols):
    groups = SUB // batch
    m = np.zeros((batch, groups, 2 * cols, cols + 2, groups, batch), np.float32)
    for g in range(groups):
        for b in range(batch):
            for c in range(cols):
                m[b, g, 2 * c, c + 1, g, b] = 0.75
                m[b, g, 2 * c, c, g, b] = 0.25
                m[b, g, 2 * c + 1, c + 1, g, b] = 0.75
                m[b, g, 2 * c + 1, c + 2, g, b] = 0.25
    return jnp.asarray(m.reshape(SUB * 2 * cols, (cols + 2) * SUB), BF)


def per_device(prev, skip_c, skip_f, cw, cb, cp, co, fw, fb, fp, fo):
    batch, hc, cc, ch = prev.shape
    _, hf, cf, _ = skip_f.shape
    groups = SUB // batch
    rc, rf = hc // groups, hf // groups

    def grouped(v):
        return v.reshape(batch, groups, v.shape[1] // groups, v.shape[2], ch)

    vmem = pl.BlockSpec(memory_space=pltpu.VMEM)
    hbm = pl.BlockSpec(memory_space=pl.ANY)
    dma = pltpu.SemaphoreType.DMA
    z = pl.pallas_call(
        functools.partial(body, batch),
        out_shape=jax.ShapeDtypeStruct((rf + 2, cf + 2, SUB, ch), BF),
        in_specs=[vmem, vmem, vmem, hbm, vmem, vmem, vmem, hbm, vmem, vmem, vmem, vmem],
        out_specs=vmem,
        scratch_shapes=[
            pltpu.VMEM((5, rc + 2, cc + 2, SUB, ch), BF),
            pltpu.VMEM((5, rf + 2, cf + 2, SUB, ch), BF),
            pltpu.VMEM((5, 2, cc // groups, SUB, ch), BF),
            pltpu.VMEM((5, 2, cf // groups, SUB, ch), BF),
            pltpu.VMEM((5, 2, cc // groups, SUB, ch), BF),
            pltpu.VMEM((5, 2, cf // groups, SUB, ch), BF),
            pltpu.VMEM((5, 4, SUB, ch), BF),
            pltpu.VMEM((5, 4, SUB, ch), BF),
            pltpu.VMEM((4, 9 * ch, ch), BF),
            pltpu.VMEM((4, 9 * ch, ch), BF),
            pltpu.VMEM((rc, cc, SUB, ch), F32),
            pltpu.VMEM((rf, cf, SUB, ch), BF),
            pltpu.VMEM((rf, cf, SUB, ch), F32),
            dma((5, 8)),
            dma((5, 8)),
            dma((5, 8)),
            dma((5, 8)),
            dma((2, 4)),
        ],
        compiler_params=pltpu.CompilerParams(
            collective_id=0, has_side_effects=True, vmem_limit_bytes=60 * 1024 * 1024
        ),
    )(
        grouped(prev),
        grouped(skip_c),
        grouped(skip_f),
        cw.reshape(4, 9 * ch, ch),
        cb,
        cp,
        co.reshape(1, ch),
        fw.reshape(4, 9 * ch, ch),
        fb,
        fp,
        regroup_matrix(batch, cc),
        regroup_matrix(batch, cf),
    )
    spread = spread_matrix(batch, cf)
    decoded = pl.pallas_call(
        functools.partial(raise_body, batch),
        grid=(rf,),
        out_shape=jax.ShapeDtypeStruct((batch, groups, 2 * rf, 2 * cf, ch), BF),
        in_specs=[
            pl.BlockSpec((rf + 2, cf + 2, SUB, ch), lambda r: (0, 0, 0, 0)),
            pl.BlockSpec(spread.shape, lambda r: (0, 0)),
            pl.BlockSpec((1, ch), lambda r: (0, 0)),
        ],
        out_specs=pl.BlockSpec((batch, groups, 2, 2 * cf, ch), lambda r: (0, 0, r, 0, 0)),
    )(z, spread, fo.reshape(1, ch))
    return decoded.reshape(batch, 2 * hf, 2 * cf, ch)


def solution(mesh):
    image = P(None, "row", "col", None)
    return jax.shard_map(
        per_device,
        mesh=mesh,
        in_specs=(image, image, image) + (P(),) * 8,
        out_specs=image,
        check_vma=False,
    )
```

```python
import functools

import jax
import jax.numpy as jnp
import numpy as np
from jax import lax
from jax.experimental import pallas as pl
from jax.experimental.pallas import tpu as pltpu
from jax.sharding import PartitionSpec as P

SUB = 16
BF = jnp.bfloat16
F32 = jnp.float32
DIRECTIONS = ((0, -1), (0, 1), (-1, 0), (1, 0), (-1, -1), (-1, 1), (1, -1), (1, 1))


def roll(value, shift):
    shift = shift % SUB
    if shift == 0:
        return value
    axis = value.ndim - 2
    if value.ndim == 3:
        return jnp.concatenate([value[:, SUB - shift :], value[:, : SUB - shift]], axis=1)
    return jnp.concatenate([value[SUB - shift :], value[: SUB - shift]], axis=axis)


class Level:
    def __init__(self, width, images, stage, packed, landed, corners, send, recv, slot):
        self.width = width
        self.image = images.at[stage]
        self.packed = packed.at[slot, :, 0:width]
        self.landed = landed.at[slot, :, 0:width]
        self.corners = corners.at[slot, :, 0:width, 0:width]
        self.send = send.at[slot]
        self.recv = recv.at[slot]
        self.rows = images.shape[1] - 2 * width
        self.cols = images.shape[2] - 2 * width


class Place:
    def __init__(self):
        self.row = lax.axis_index("row")
        self.col = lax.axis_index("col")
        self.rows = lax.axis_size("row")
        self.cols = lax.axis_size("col")

    def has(self, dr, dc):
        ok = None
        tests = []
        if dr == -1:
            tests.append(self.row > 0)
        if dr == 1:
            tests.append(self.row < self.rows - 1)
        if dc == -1:
            tests.append(self.col > 0)
        if dc == 1:
            tests.append(self.col < self.cols - 1)
        for test in tests:
            ok = test if ok is None else jnp.logical_and(ok, test)
        return ok

    def peers(self):
        def around(index, count):
            return 1 + (index > 0).astype(jnp.int32) + (index < count - 1).astype(jnp.int32)

        return around(self.row, self.rows) * around(self.col, self.cols) - 1

    def edges(self):
        return (
            self.row == 0,
            self.row == self.rows - 1,
            self.col == 0,
            self.col == self.cols - 1,
        )

    def at(self, dr, dc):
        return (self.row + dr, self.col + dc)


def sub_index(shape):
    return lax.broadcasted_iota(jnp.int32, shape, len(shape) - 2)


def copies(place, lv):
    r, c, h = lv.rows, lv.cols, lv.width
    im = lv.image
    inner = pl.ds(h, r)
    low, high_r, high_c = pl.ds(h, h), pl.ds(r, h), pl.ds(c, h)
    ends = (
        (im.at[inner, low], im.at[inner, pl.ds(c + h, h)]),
        (im.at[inner, high_c], im.at[inner, pl.ds(0, h)]),
        (lv.packed.at[0], lv.landed.at[1]),
        (lv.packed.at[1], lv.landed.at[0]),
        (im.at[low, low], lv.corners.at[3]),
        (im.at[low, high_c], lv.corners.at[2]),
        (im.at[high_r, low], lv.corners.at[1]),
        (im.at[high_r, high_c], lv.corners.at[0]),
    )
    return [
        pltpu.make_async_remote_copy(
            src_ref=src,
            dst_ref=dst,
            send_sem=lv.send.at[i],
            recv_sem=lv.recv.at[i],
            device_id=place.at(*DIRECTIONS[i]),
            device_id_type=pl.DeviceIdType.MESH,
        )
        for i, (src, dst) in enumerate(ends)
    ]


def exchange(place, lv, batch):
    r, c, h = lv.rows, lv.cols, lv.width
    groups = SUB // batch
    channels = lv.image.shape[-1]
    moves = copies(place, lv)
    for i in (4, 5, 6, 7, 0, 1):
        pl.when(place.has(*DIRECTIONS[i]))(moves[i].start)
    slot = sub_index((c // groups, SUB, channels)) // batch
    for side in (0, 1):
        for k in range(h):
            row = h + k if side == 0 else r + k
            v = lv.image[row, h : c + h].astype(F32).reshape(c // groups, groups, SUB, channels)
            total = None
            for q in range(groups):
                part = roll(v[:, q], batch * (q if side == 0 else q + 1))
                total = part if total is None else jnp.where(slot == q, part, total)
            lv.packed[side, k] = total.astype(BF)
        pl.when(place.has(*DIRECTIONS[2 + side]))(moves[2 + side].start)


def settle(place, lv, batch, replicate):
    r, c, h = lv.rows, lv.cols, lv.width
    im, landed, corners = lv.image, lv.landed, lv.corners
    groups = SUB // batch
    channels = im.shape[-1]
    moves = copies(place, lv)
    for i, (dr, dc) in enumerate(DIRECTIONS):
        pl.when(place.has(dr, dc))(moves[i].wait_send)
        pl.when(place.has(-dr, -dc))(moves[i].wait_recv)

    no_up, no_down, no_left, no_right = place.edges()

    def rolled(tile, shift):
        return roll(tile.astype(F32), shift).astype(BF)

    for missing, at, edge in ((no_left, 0, h), (no_right, c + h, c)):

        @pl.when(missing)
        def _(at=at, edge=edge):
            if replicate:
                im[h : r + h, at : at + h] = im[h : r + h, edge : edge + h]
            else:
                im[h : r + h, at : at + h] = jnp.zeros((r, h, SUB, channels), BF)

    for side, missing in ((0, no_up), (1, no_down)):

        @pl.when(missing)
        def _(side=side):
            if replicate:
                landed[side] = lv.packed[side]
            else:
                landed[side] = jnp.zeros((h, c // groups, SUB, channels), BF)

    last = c // groups - 1
    for k, vertical, horizontal in (
        (0, no_up, no_left),
        (1, no_up, no_right),
        (2, no_down, no_left),
        (3, no_down, no_right),
    ):
        if not replicate:

            @pl.when(jnp.logical_or(vertical, horizontal))
            def _(k=k):
                corners[k] = jnp.zeros((h, h, SUB, channels), BF)

        else:
            side = k // 2
            turn = -batch if side == 0 else batch
            row = 1 if side == 0 else r
            col = 0 if k % 2 == 0 else c + 1

            @pl.when(vertical)
            def _(k=k, turn=turn, row=row, col=col):
                corners[k, 0, 0] = rolled(im[row, col], turn)

            shift = (-batch, 0, 0, batch)[k]
            block = 0 if k % 2 == 0 else last

            @pl.when(jnp.logical_and(jnp.logical_not(vertical), horizontal))
            def _(k=k, side=side, shift=shift, block=block):
                corners[k, 0, 0] = rolled(landed[side, 0, block], shift)

    group = sub_index((c + 2 * h, SUB, channels)) // batch
    for side in (0, 1):
        turn = batch if side == 0 else -batch
        chosen = 0 if side == 0 else groups - 1
        for k in range(h):
            near = roll(im[r + k if side == 0 else h + k].astype(F32), turn)
            wide = landed[side, k].astype(F32)
            parts = [
                roll(wide, -batch * q if side == 0 else batch * (groups - 1 - q))
                for q in range(groups)
            ]
            inner = jnp.stack(parts, axis=1).reshape(c, SUB, channels)
            ends = [roll(corners[2 * side + e, k].astype(F32), turn) for e in (0, 1)]
            outer = jnp.concatenate([ends[0], inner, ends[1]], axis=0)
            to = k if side == 0 else r + h + k
            im[to] = jnp.where(group == chosen, outer, near).astype(BF)


def clear_outside(place, ref, batch):
    rows, cols, _, channels = ref.shape
    no_up, no_down, no_left, no_right = place.edges()
    for missing, at in ((no_left, 0), (no_right, cols - 1)):

        @pl.when(missing)
        def _(at=at):
            ref[:, at] = jnp.zeros((rows, SUB, channels), BF)

    group = sub_index((cols, SUB, channels)) // batch
    for missing, at, chosen in ((no_up, 0, 0), (no_down, rows - 1, SUB // batch - 1)):

        @pl.when(missing)
        def _(at=at, chosen=chosen):
            ref[at] = jnp.where(group == chosen, 0.0, ref[at].astype(F32)).astype(BF)


def conv_rows(image, weight, start, count):
    c = image.shape[1] - 2
    channels = image.shape[-1]
    taps = [
        image[pl.ds(start + dr, count), dc : dc + c].reshape(count * c * SUB, channels)
        for dr in range(3)
        for dc in range(3)
    ]
    v = jnp.dot(jnp.concatenate(taps, axis=1), weight[...], preferred_element_type=F32)
    return v


def body(
    batch,
    prev,
    skip_c,
    skip_f,
    cw_hbm,
    cb,
    cp,
    co,
    fw_hbm,
    fb,
    fp,
    perm_c,
    perm_f,
    out,
    ic,
    if_,
    hid_c,
    hid_f,
    up_c,
    up_f,
    pack_c,
    pack_f,
    land_c,
    land_f,
    corner_c,
    corner_f,
    cw,
    fw,
    xc,
    xf,
    sum_f,
    send_c,
    recv_c,
    send_f,
    recv_f,
    wsem,
):
    place = Place()
    channels = skip_c.shape[-1]
    loads = {}
    for i in range(4):
        for k, (src, dst) in enumerate(((cw_hbm, cw), (fw_hbm, fw))):
            loads[k, i] = pltpu.make_async_copy(src.at[i], dst.at[i], wsem.at[k, i])
    for key in ((0, 0), (0, 1), (1, 0), (0, 2), (0, 3), (1, 1), (1, 2), (1, 3)):
        loads[key].start()

    barrier = pltpu.get_barrier_semaphore()
    for d in DIRECTIONS:

        @pl.when(place.has(*d))
        def _(d=d):
            pl.semaphore_signal(
                barrier, inc=1, device_id=place.at(*d), device_id_type=pl.DeviceIdType.MESH
            )

    side_c = (pack_c, land_c, corner_c, send_c, recv_c)
    side_f = (pack_f, land_f, corner_f, send_f, recv_f)
    lc = [Level(2, ic, 0, *side_c, 0), Level(2, ic, 1, *side_c, 1), Level(1, up_c, 0, *side_c, 2)]
    lf = [Level(2, if_, 0, *side_f, 0), Level(2, if_, 1, *side_f, 1), Level(1, up_f, 0, *side_f, 2)]
    rc, cc, rf, cf = lc[0].rows, lc[0].cols, lf[0].rows, lf[0].cols

    def regroup(ref, perm, row):
        tile = ref[:, :, row].reshape(perm.shape[0], channels)
        return jnp.dot(perm[...], tile, preferred_element_type=F32).reshape(-1, SUB, channels)

    @pl.loop(0, rc)
    def _(row):
        v = regroup(skip_c, perm_c, row)
        xc[row] = v + regroup(prev, perm_c, row)
        ic[0, row + 2, 2 : cc + 2] = jnp.maximum(v, 0.0).astype(BF)

    pl.semaphore_wait(barrier, place.peers())

    exchange(place, lc[0], batch)

    @pl.loop(0, rf)
    def _(row):
        v = regroup(skip_f, perm_f, row)
        xf[row] = v.astype(BF)
        if_[0, row + 2, 2 : cf + 2] = jnp.maximum(v, 0.0).astype(BF)

    exchange(place, lf[0], batch)

    def coarse(stage, finish):
        settle(place, lc[stage], batch, False)
        first = 2 * stage
        loads[0, first].wait()
        v = conv_rows(lc[stage].image, cw.at[first], 0, rc + 2) + cb[first : first + 1]
        hid_c[...] = jnp.maximum(v, 0.0).astype(BF).reshape(rc + 2, cc + 2, SUB, channels)
        clear_outside(place, hid_c, batch)
        loads[0, first + 1].wait()
        v = conv_rows(hid_c, cw.at[first + 1], 0, rc) + cb[first + 1 : first + 2]
        lc[stage + 1].image[finish[0] : finish[0] + rc, finish[0] : finish[0] + cc] = finish[1](
            v.reshape(rc, cc, SUB, channels)
        )
        exchange(place, lc[stage + 1], batch)

    step = 2 if rf % 2 == 0 else 1

    def fine_hidden(stage):
        settle(place, lf[stage], batch, False)
        first = 2 * stage
        loads[1, first].wait()

        @pl.loop(0, (rf + 2) // step)
        def _(i):
            v = conv_rows(lf[stage].image, fw.at[first], i * step, step) + fb[first : first + 1]
            v = jnp.maximum(v, 0.0).astype(BF)
            hid_f[pl.ds(i * step, step)] = v.reshape(step, cf + 2, SUB, channels)

        clear_outside(place, hid_f, batch)

    def fine_final(stage, finish):
        second = 2 * stage + 1
        loads[1, second].wait()

        @pl.loop(0, rf // step)
        def _(i):
            v = conv_rows(hid_f, fw.at[second], i * step, step) + fb[second : second + 1]
            finish(i * step, v.reshape(step, cf, SUB, channels))

    def summed(v):
        v = v + xc[...]
        xc[...] = v
        return jnp.maximum(v, 0.0).astype(BF)

    def lifted(v):
        top = (v + xc[...]).astype(BF).reshape(rc * cc * SUB, channels)
        z = jnp.dot(top, cp[...], preferred_element_type=F32)
        return z.astype(BF).reshape(rc, cc, SUB, channels)

    def keep_unit(row, v):
        sum_f[pl.ds(row, step)] = v + xf[pl.ds(row, step)].astype(F32)

    def keep_top(row, v):
        top = (v + sum_f[pl.ds(row, step)]).astype(BF).reshape(step * cf * SUB, channels)
        z = jnp.dot(top, fp[...], preferred_element_type=F32)
        up_f[0, pl.ds(row + 1, step), 1 : cf + 1] = z.astype(BF).reshape(step, cf, SUB, channels)

    coarse(0, (2, summed))
    fine_hidden(0)
    coarse(1, (1, lifted))
    fine_final(0, keep_unit)
    settle(place, lc[2], batch, True)

    @pl.loop(0, rc)
    def _(row):
        mid = 0.75 * up_c[0, row + 1].astype(F32)
        for p in range(2):
            v = mid + 0.25 * up_c[0, row + 2 * p].astype(F32)
            core = 0.75 * v[1 : cc + 1]
            even = core + 0.25 * v[0:cc]
            odd = core + 0.25 * v[2 : cc + 2]
            both = jnp.stack([even, odd], axis=1).reshape(cf, SUB, channels)
            joined = (both + co[...]).astype(BF).astype(F32)
            total = joined + sum_f[2 * row + p]
            sum_f[2 * row + p] = total
            if_[1, 2 * row + p + 2, 2 : cf + 2] = jnp.maximum(total, 0.0).astype(BF)

    exchange(place, lf[1], batch)
    fine_hidden(1)
    fine_final(1, keep_top)
    exchange(place, lf[2], batch)
    settle(place, lf[2], batch, True)

    @pl.loop(0, rf + 2)
    def _(row):
        out[row] = up_f[0, row]


def raise_body(batch, z, spread, offset, out):
    row = pl.program_id(0)
    channels = z.shape[-1]
    mid = 0.75 * z[row + 1].astype(F32)
    for p in range(2):
        v = (mid + 0.25 * z[row + 2 * p].astype(F32)).astype(BF).reshape(-1, channels)
        res = jnp.dot(spread[...], v, preferred_element_type=F32) + offset[...]
        out[:, :, p] = res.astype(BF).reshape(batch, SUB // batch, -1, channels)


def regroup_matrix(batch, cols):
    groups = SUB // batch
    m = np.zeros((cols, groups, batch, batch, groups, cols), np.float32)
    for c in range(cols):
        for g in range(groups):
            for b in range(batch):
                m[c, g, b, b, g, c] = 1.0
    return jnp.asarray(m.reshape(cols * SUB, cols * SUB), BF)


def spread_matrix(batch, cols):
    groups = SUB // batch
    m = np.zeros((batch, groups, 2 * cols, cols + 2, groups, batch), np.float32)
    for g in range(groups):
        for b in range(batch):
            for c in range(cols):
                m[b, g, 2 * c, c + 1, g, b] = 0.75
                m[b, g, 2 * c, c, g, b] = 0.25
                m[b, g, 2 * c + 1, c + 1, g, b] = 0.75
                m[b, g, 2 * c + 1, c + 2, g, b] = 0.25
    return jnp.asarray(m.reshape(SUB * 2 * cols, (cols + 2) * SUB), BF)


def per_device(prev, skip_c, skip_f, cw, cb, cp, co, fw, fb, fp, fo):
    batch, hc, cc, ch = prev.shape
    _, hf, cf, _ = skip_f.shape
    groups = SUB // batch
    rc, rf = hc // groups, hf // groups

    def grouped(v):
        return v.reshape(batch, groups, v.shape[1] // groups, v.shape[2], ch)

    vmem = pl.BlockSpec(memory_space=pltpu.VMEM)
    hbm = pl.BlockSpec(memory_space=pl.ANY)
    dma = pltpu.SemaphoreType.DMA
    z = pl.pallas_call(
        functools.partial(body, batch),
        out_shape=jax.ShapeDtypeStruct((rf + 2, cf + 2, SUB, ch), BF),
        in_specs=[vmem, vmem, vmem, hbm, vmem, vmem, vmem, hbm, vmem, vmem, vmem, vmem],
        out_specs=vmem,
        scratch_shapes=[
            pltpu.VMEM((2, rc + 4, cc + 4, SUB, ch), BF),
            pltpu.VMEM((2, rf + 4, cf + 4, SUB, ch), BF),
            pltpu.VMEM((rc + 2, cc + 2, SUB, ch), BF),
            pltpu.VMEM((rf + 2, cf + 2, SUB, ch), BF),
            pltpu.VMEM((1, rc + 2, cc + 2, SUB, ch), BF),
            pltpu.VMEM((1, rf + 2, cf + 2, SUB, ch), BF),
            pltpu.VMEM((3, 2, 2, cc // groups, SUB, ch), BF),
            pltpu.VMEM((3, 2, 2, cf // groups, SUB, ch), BF),
            pltpu.VMEM((3, 2, 2, cc // groups, SUB, ch), BF),
            pltpu.VMEM((3, 2, 2, cf // groups, SUB, ch), BF),
            pltpu.VMEM((3, 4, 2, 2, SUB, ch), BF),
            pltpu.VMEM((3, 4, 2, 2, SUB, ch), BF),
            pltpu.VMEM((4, 9 * ch, ch), BF),
            pltpu.VMEM((4, 9 * ch, ch), BF),
            pltpu.VMEM((rc, cc, SUB, ch), F32),
            pltpu.VMEM((rf, cf, SUB, ch), BF),
            pltpu.VMEM((rf, cf, SUB, ch), F32),
            dma((3, 8)),
            dma((3, 8)),
            dma((3, 8)),
            dma((3, 8)),
            dma((2, 4)),
        ],
        compiler_params=pltpu.CompilerParams(
            collective_id=0, has_side_effects=True, vmem_limit_bytes=60 * 1024 * 1024
        ),
    )(
        grouped(prev),
        grouped(skip_c),
        grouped(skip_f),
        cw.reshape(4, 9 * ch, ch),
        cb,
        cp,
        co.reshape(1, ch),
        fw.reshape(4, 9 * ch, ch),
        fb,
        fp,
        regroup_matrix(batch, cc),
        regroup_matrix(batch, cf),
    )
    spread = spread_matrix(batch, cf)
    decoded = pl.pallas_call(
        functools.partial(raise_body, batch),
        grid=(rf,),
        out_shape=jax.ShapeDtypeStruct((batch, groups, 2 * rf, 2 * cf, ch), BF),
        in_specs=[
            pl.BlockSpec((rf + 2, cf + 2, SUB, ch), lambda r: (0, 0, 0, 0)),
            pl.BlockSpec(spread.shape, lambda r: (0, 0)),
            pl.BlockSpec((1, ch), lambda r: (0, 0)),
        ],
        out_specs=pl.BlockSpec((batch, groups, 2, 2 * cf, ch), lambda r: (0, 0, r, 0, 0)),
    )(z, spread, fo.reshape(1, ch))
    return decoded.reshape(batch, 2 * hf, 2 * cf, ch)


def solution(mesh):
    image = P(None, "row", "col", None)
    return jax.shard_map(
        per_device,
        mesh=mesh,
        in_specs=(image, image, image) + (P(),) * 8,
        out_specs=image,
        check_vma=False,
    )
```

```python
import functools

import jax
import jax.numpy as jnp
import numpy as np
from jax import lax
from jax.experimental import pallas as pl
from jax.experimental.pallas import tpu as pltpu
from jax.sharding import PartitionSpec as P

SUB = 16
BF = jnp.bfloat16
F32 = jnp.float32
DIRECTIONS = ((0, -1), (0, 1), (-1, 0), (1, 0), (-1, -1), (-1, 1), (1, -1), (1, 1))


def roll(value, shift):
    shift = shift % SUB
    if shift == 0:
        return value
    axis = value.ndim - 2
    if value.ndim == 3:
        return jnp.concatenate([value[:, SUB - shift :], value[:, : SUB - shift]], axis=1)
    return jnp.concatenate([value[SUB - shift :], value[: SUB - shift]], axis=axis)


class Level:
    def __init__(self, width, images, stage, packed, landed, corners, send, recv, slot):
        self.width = width
        self.image = images.at[stage]
        self.packed = packed.at[slot, :, 0:width]
        self.landed = landed.at[slot, :, 0:width]
        self.corners = corners.at[slot, :, 0:width, 0:width]
        self.send = send.at[slot]
        self.recv = recv.at[slot]
        self.rows = images.shape[1] - 2 * width
        self.cols = images.shape[2] - 2 * width


class Place:
    def __init__(self):
        self.row = lax.axis_index("row")
        self.col = lax.axis_index("col")
        self.rows = lax.axis_size("row")
        self.cols = lax.axis_size("col")

    def has(self, dr, dc):
        ok = None
        tests = []
        if dr == -1:
            tests.append(self.row > 0)
        if dr == 1:
            tests.append(self.row < self.rows - 1)
        if dc == -1:
            tests.append(self.col > 0)
        if dc == 1:
            tests.append(self.col < self.cols - 1)
        for test in tests:
            ok = test if ok is None else jnp.logical_and(ok, test)
        return ok

    def peers(self):
        def around(index, count):
            return 1 + (index > 0).astype(jnp.int32) + (index < count - 1).astype(jnp.int32)

        return around(self.row, self.rows) * around(self.col, self.cols) - 1

    def edges(self):
        return (
            self.row == 0,
            self.row == self.rows - 1,
            self.col == 0,
            self.col == self.cols - 1,
        )

    def at(self, dr, dc):
        return (self.row + dr, self.col + dc)


def sub_index(shape):
    return lax.broadcasted_iota(jnp.int32, shape, len(shape) - 2)


def copies(place, lv):
    r, c, h = lv.rows, lv.cols, lv.width
    im = lv.image
    inner = pl.ds(h, r)
    low, high_r, high_c = pl.ds(h, h), pl.ds(r, h), pl.ds(c, h)
    ends = (
        (im.at[inner, low], im.at[inner, pl.ds(c + h, h)]),
        (im.at[inner, high_c], im.at[inner, pl.ds(0, h)]),
        (lv.packed.at[0], lv.landed.at[1]),
        (lv.packed.at[1], lv.landed.at[0]),
        (im.at[low, low], lv.corners.at[3]),
        (im.at[low, high_c], lv.corners.at[2]),
        (im.at[high_r, low], lv.corners.at[1]),
        (im.at[high_r, high_c], lv.corners.at[0]),
    )
    return [
        pltpu.make_async_remote_copy(
            src_ref=src,
            dst_ref=dst,
            send_sem=lv.send.at[i],
            recv_sem=lv.recv.at[i],
            device_id=place.at(*DIRECTIONS[i]),
            device_id_type=pl.DeviceIdType.MESH,
        )
        for i, (src, dst) in enumerate(ends)
    ]


def exchange(place, lv, batch):
    r, c, h = lv.rows, lv.cols, lv.width
    groups = SUB // batch
    channels = lv.image.shape[-1]
    moves = copies(place, lv)
    for i in (4, 5, 6, 7, 0, 1):
        pl.when(place.has(*DIRECTIONS[i]))(moves[i].start)
    slot = sub_index((c // groups, SUB, channels)) // batch
    for side in (0, 1):
        for k in range(h):
            row = h + k if side == 0 else r + k
            v = lv.image[row, h : c + h].astype(F32).reshape(c // groups, groups, SUB, channels)
            total = None
            for q in range(groups):
                part = roll(v[:, q], batch * (q if side == 0 else q + 1))
                total = part if total is None else jnp.where(slot == q, part, total)
            lv.packed[side, k] = total.astype(BF)
        pl.when(place.has(*DIRECTIONS[2 + side]))(moves[2 + side].start)


def settle(place, lv, batch, replicate):
    r, c, h = lv.rows, lv.cols, lv.width
    im, landed, corners = lv.image, lv.landed, lv.corners
    groups = SUB // batch
    channels = im.shape[-1]
    moves = copies(place, lv)
    for i, (dr, dc) in enumerate(DIRECTIONS):
        pl.when(place.has(dr, dc))(moves[i].wait_send)
        pl.when(place.has(-dr, -dc))(moves[i].wait_recv)

    no_up, no_down, no_left, no_right = place.edges()

    def rolled(tile, shift):
        return roll(tile.astype(F32), shift).astype(BF)

    for missing, at, edge in ((no_left, 0, h), (no_right, c + h, c)):

        @pl.when(missing)
        def _(at=at, edge=edge):
            if replicate:
                im[h : r + h, at : at + h] = im[h : r + h, edge : edge + h]
            else:
                im[h : r + h, at : at + h] = jnp.zeros((r, h, SUB, channels), BF)

    for side, missing in ((0, no_up), (1, no_down)):

        @pl.when(missing)
        def _(side=side):
            if replicate:
                landed[side] = lv.packed[side]
            else:
                landed[side] = jnp.zeros((h, c // groups, SUB, channels), BF)

    last = c // groups - 1
    for k, vertical, horizontal in (
        (0, no_up, no_left),
        (1, no_up, no_right),
        (2, no_down, no_left),
        (3, no_down, no_right),
    ):
        if not replicate:

            @pl.when(jnp.logical_or(vertical, horizontal))
            def _(k=k):
                corners[k] = jnp.zeros((h, h, SUB, channels), BF)

        else:
            side = k // 2
            turn = -batch if side == 0 else batch
            row = 1 if side == 0 else r
            col = 0 if k % 2 == 0 else c + 1

            @pl.when(vertical)
            def _(k=k, turn=turn, row=row, col=col):
                corners[k, 0, 0] = rolled(im[row, col], turn)

            shift = (-batch, 0, 0, batch)[k]
            block = 0 if k % 2 == 0 else last

            @pl.when(jnp.logical_and(jnp.logical_not(vertical), horizontal))
            def _(k=k, side=side, shift=shift, block=block):
                corners[k, 0, 0] = rolled(landed[side, 0, block], shift)

    group = sub_index((c + 2 * h, SUB, channels)) // batch
    for side in (0, 1):
        turn = batch if side == 0 else -batch
        chosen = 0 if side == 0 else groups - 1
        for k in range(h):
            near = roll(im[r + k if side == 0 else h + k].astype(F32), turn)
            wide = landed[side, k].astype(F32)
            parts = [
                roll(wide, -batch * q if side == 0 else batch * (groups - 1 - q))
                for q in range(groups)
            ]
            inner = jnp.stack(parts, axis=1).reshape(c, SUB, channels)
            ends = [roll(corners[2 * side + e, k].astype(F32), turn) for e in (0, 1)]
            outer = jnp.concatenate([ends[0], inner, ends[1]], axis=0)
            to = k if side == 0 else r + h + k
            im[to] = jnp.where(group == chosen, outer, near).astype(BF)


def clear_outside(place, ref, batch):
    rows, cols, _, channels = ref.shape
    no_up, no_down, no_left, no_right = place.edges()
    for missing, at in ((no_left, 0), (no_right, cols - 1)):

        @pl.when(missing)
        def _(at=at):
            ref[:, at] = jnp.zeros((rows, SUB, channels), BF)

    group = sub_index((cols, SUB, channels)) // batch
    for missing, at, chosen in ((no_up, 0, 0), (no_down, rows - 1, SUB // batch - 1)):

        @pl.when(missing)
        def _(at=at, chosen=chosen):
            ref[at] = jnp.where(group == chosen, 0.0, ref[at].astype(F32)).astype(BF)


def conv_rows(image, weight, start, count, spans=None):
    channels = image.shape[-1]
    spans = spans or ((0, image.shape[1] - 2),)
    taps = [
        jnp.concatenate(
            [
                image[pl.ds(start + dr, count), at + dc : at + dc + n].reshape(-1, channels)
                for at, n in spans
            ],
            axis=0,
        )
        for dr in range(3)
        for dc in range(3)
    ]
    return jnp.dot(jnp.concatenate(taps, axis=1), weight[...], preferred_element_type=F32)


def body(
    batch,
    prev,
    skip_c,
    skip_f,
    cw_hbm,
    cb,
    cp,
    co,
    fw_hbm,
    fb,
    fp,
    perm_c,
    perm_f,
    out,
    ic,
    if_,
    hid_c,
    hid_f,
    up_c,
    up_f,
    pack_c,
    pack_f,
    land_c,
    land_f,
    corner_c,
    corner_f,
    cw,
    fw,
    xc,
    xf,
    sum_f,
    send_c,
    recv_c,
    send_f,
    recv_f,
    wsem,
):
    place = Place()
    channels = skip_c.shape[-1]
    loads = {}
    for i in range(4):
        for k, (src, dst) in enumerate(((cw_hbm, cw), (fw_hbm, fw))):
            loads[k, i] = pltpu.make_async_copy(src.at[i], dst.at[i], wsem.at[k, i])
    for key in ((0, 0), (0, 1), (1, 0), (0, 2), (0, 3), (1, 1), (1, 2), (1, 3)):
        loads[key].start()

    barrier = pltpu.get_barrier_semaphore()
    for d in DIRECTIONS:

        @pl.when(place.has(*d))
        def _(d=d):
            pl.semaphore_signal(
                barrier, inc=1, device_id=place.at(*d), device_id_type=pl.DeviceIdType.MESH
            )

    side_c = (pack_c, land_c, corner_c, send_c, recv_c)
    side_f = (pack_f, land_f, corner_f, send_f, recv_f)
    lc = [Level(2, ic, 0, *side_c, 0), Level(2, ic, 1, *side_c, 1), Level(1, up_c, 0, *side_c, 2)]
    lf = [Level(2, if_, 0, *side_f, 0), Level(2, if_, 1, *side_f, 1), Level(1, up_f, 0, *side_f, 2)]
    rc, cc, rf, cf = lc[0].rows, lc[0].cols, lf[0].rows, lf[0].cols

    def regroup(ref, perm, row):
        tile = ref[:, :, row].reshape(perm.shape[0], channels)
        return jnp.dot(perm[...], tile, preferred_element_type=F32).reshape(-1, SUB, channels)

    @pl.loop(0, rc)
    def _(row):
        v = regroup(skip_c, perm_c, row)
        xc[row] = v + regroup(prev, perm_c, row)
        ic[0, row + 2, 2 : cc + 2] = jnp.maximum(v, 0.0).astype(BF)

    pl.semaphore_wait(barrier, place.peers())

    exchange(place, lc[0], batch)

    @pl.loop(0, rf)
    def _(row):
        v = regroup(skip_f, perm_f, row)
        xf[row] = v.astype(BF)
        if_[0, row + 2, 2 : cf + 2] = jnp.maximum(v, 0.0).astype(BF)

    exchange(place, lf[0], batch)

    def coarse(stage, finish):
        settle(place, lc[stage], batch, False)
        first = 2 * stage
        loads[0, first].wait()
        v = conv_rows(lc[stage].image, cw.at[first], 0, rc + 2) + cb[first : first + 1]
        hid_c[...] = jnp.maximum(v, 0.0).astype(BF).reshape(rc + 2, cc + 2, SUB, channels)
        clear_outside(place, hid_c, batch)
        loads[0, first + 1].wait()
        v = conv_rows(hid_c, cw.at[first + 1], 0, rc) + cb[first + 1 : first + 2]
        lc[stage + 1].image[finish[0] : finish[0] + rc, finish[0] : finish[0] + cc] = finish[1](
            v.reshape(rc, cc, SUB, channels)
        )
        exchange(place, lc[stage + 1], batch)

    step = 2 if rf % 2 == 0 else 1

    def fine_hidden(stage):
        first = 2 * stage

        def compute(start, count, spans):
            v = conv_rows(lf[stage].image, fw.at[first], start, count, spans)
            v = jnp.maximum(v + fb[first : first + 1], 0.0).astype(BF)
            done = 0
            for at, n in spans:
                size = count * n * SUB
                part = v[done : done + size].reshape(count, n, SUB, channels)
                hid_f[pl.ds(start, count), at : at + n] = part
                done += size

        loads[1, first].wait()

        @pl.loop(0, (rf - 2) // step)
        def _(i):
            compute(2 + i * step, step, ((2, cf - 2),))

        settle(place, lf[stage], batch, False)

        @pl.loop(0, 2)
        def _(i):
            compute(i * rf, 2, ((0, cf + 2),))

        compute(2, rf - 2, ((0, 2), (cf, 2)))
        clear_outside(place, hid_f, batch)

    def fine_final(stage, finish):
        second = 2 * stage + 1
        loads[1, second].wait()

        @pl.loop(0, rf // step)
        def _(i):
            v = conv_rows(hid_f, fw.at[second], i * step, step) + fb[second : second + 1]
            finish(i * step, v.reshape(step, cf, SUB, channels))

    def summed(v):
        v = v + xc[...]
        xc[...] = v
        return jnp.maximum(v, 0.0).astype(BF)

    def lifted(v):
        top = (v + xc[...]).astype(BF).reshape(rc * cc * SUB, channels)
        z = jnp.dot(top, cp[...], preferred_element_type=F32)
        return z.astype(BF).reshape(rc, cc, SUB, channels)

    def keep_unit(row, v):
        sum_f[pl.ds(row, step)] = v + xf[pl.ds(row, step)].astype(F32)

    def keep_top(row, v):
        top = (v + sum_f[pl.ds(row, step)]).astype(BF).reshape(step * cf * SUB, channels)
        z = jnp.dot(top, fp[...], preferred_element_type=F32)
        up_f[0, pl.ds(row + 1, step), 1 : cf + 1] = z.astype(BF).reshape(step, cf, SUB, channels)

    coarse(0, (2, summed))
    fine_hidden(0)
    coarse(1, (1, lifted))
    fine_final(0, keep_unit)
    settle(place, lc[2], batch, True)

    @pl.loop(0, rc)
    def _(row):
        mid = 0.75 * up_c[0, row + 1].astype(F32)
        for p in range(2):
            v = mid + 0.25 * up_c[0, row + 2 * p].astype(F32)
            core = 0.75 * v[1 : cc + 1]
            even = core + 0.25 * v[0:cc]
            odd = core + 0.25 * v[2 : cc + 2]
            both = jnp.stack([even, odd], axis=1).reshape(cf, SUB, channels)
            joined = (both + co[...]).astype(BF).astype(F32)
            total = joined + sum_f[2 * row + p]
            sum_f[2 * row + p] = total
            if_[1, 2 * row + p + 2, 2 : cf + 2] = jnp.maximum(total, 0.0).astype(BF)

    exchange(place, lf[1], batch)
    fine_hidden(1)
    fine_final(1, keep_top)
    exchange(place, lf[2], batch)
    settle(place, lf[2], batch, True)

    @pl.loop(0, rf + 2)
    def _(row):
        out[row] = up_f[0, row]


def raise_body(batch, z, spread, offset, out):
    row = pl.program_id(0)
    channels = z.shape[-1]
    mid = 0.75 * z[row + 1].astype(F32)
    for p in range(2):
        v = (mid + 0.25 * z[row + 2 * p].astype(F32)).astype(BF).reshape(-1, channels)
        res = jnp.dot(spread[...], v, preferred_element_type=F32) + offset[...]
        out[:, :, p] = res.astype(BF).reshape(batch, SUB // batch, -1, channels)


def regroup_matrix(batch, cols):
    groups = SUB // batch
    m = np.zeros((cols, groups, batch, batch, groups, cols), np.float32)
    for c in range(cols):
        for g in range(groups):
            for b in range(batch):
                m[c, g, b, b, g, c] = 1.0
    return jnp.asarray(m.reshape(cols * SUB, cols * SUB), BF)


def spread_matrix(batch, cols):
    groups = SUB // batch
    m = np.zeros((batch, groups, 2 * cols, cols + 2, groups, batch), np.float32)
    for g in range(groups):
        for b in range(batch):
            for c in range(cols):
                m[b, g, 2 * c, c + 1, g, b] = 0.75
                m[b, g, 2 * c, c, g, b] = 0.25
                m[b, g, 2 * c + 1, c + 1, g, b] = 0.75
                m[b, g, 2 * c + 1, c + 2, g, b] = 0.25
    return jnp.asarray(m.reshape(SUB * 2 * cols, (cols + 2) * SUB), BF)


def per_device(prev, skip_c, skip_f, cw, cb, cp, co, fw, fb, fp, fo):
    batch, hc, cc, ch = prev.shape
    _, hf, cf, _ = skip_f.shape
    groups = SUB // batch
    rc, rf = hc // groups, hf // groups

    def grouped(v):
        return v.reshape(batch, groups, v.shape[1] // groups, v.shape[2], ch)

    vmem = pl.BlockSpec(memory_space=pltpu.VMEM)
    hbm = pl.BlockSpec(memory_space=pl.ANY)
    dma = pltpu.SemaphoreType.DMA
    z = pl.pallas_call(
        functools.partial(body, batch),
        out_shape=jax.ShapeDtypeStruct((rf + 2, cf + 2, SUB, ch), BF),
        in_specs=[vmem, vmem, vmem, hbm, vmem, vmem, vmem, hbm, vmem, vmem, vmem, vmem],
        out_specs=vmem,
        scratch_shapes=[
            pltpu.VMEM((2, rc + 4, cc + 4, SUB, ch), BF),
            pltpu.VMEM((2, rf + 4, cf + 4, SUB, ch), BF),
            pltpu.VMEM((rc + 2, cc + 2, SUB, ch), BF),
            pltpu.VMEM((rf + 2, cf + 2, SUB, ch), BF),
            pltpu.VMEM((1, rc + 2, cc + 2, SUB, ch), BF),
            pltpu.VMEM((1, rf + 2, cf + 2, SUB, ch), BF),
            pltpu.VMEM((3, 2, 2, cc // groups, SUB, ch), BF),
            pltpu.VMEM((3, 2, 2, cf // groups, SUB, ch), BF),
            pltpu.VMEM((3, 2, 2, cc // groups, SUB, ch), BF),
            pltpu.VMEM((3, 2, 2, cf // groups, SUB, ch), BF),
            pltpu.VMEM((3, 4, 2, 2, SUB, ch), BF),
            pltpu.VMEM((3, 4, 2, 2, SUB, ch), BF),
            pltpu.VMEM((4, 9 * ch, ch), BF),
            pltpu.VMEM((4, 9 * ch, ch), BF),
            pltpu.VMEM((rc, cc, SUB, ch), F32),
            pltpu.VMEM((rf, cf, SUB, ch), BF),
            pltpu.VMEM((rf, cf, SUB, ch), F32),
            dma((3, 8)),
            dma((3, 8)),
            dma((3, 8)),
            dma((3, 8)),
            dma((2, 4)),
        ],
        compiler_params=pltpu.CompilerParams(
            collective_id=0, has_side_effects=True, vmem_limit_bytes=60 * 1024 * 1024
        ),
    )(
        grouped(prev),
        grouped(skip_c),
        grouped(skip_f),
        cw.reshape(4, 9 * ch, ch),
        cb,
        cp,
        co.reshape(1, ch),
        fw.reshape(4, 9 * ch, ch),
        fb,
        fp,
        regroup_matrix(batch, cc),
        regroup_matrix(batch, cf),
    )
    spread = spread_matrix(batch, cf)
    decoded = pl.pallas_call(
        functools.partial(raise_body, batch),
        grid=(rf,),
        out_shape=jax.ShapeDtypeStruct((batch, groups, 2 * rf, 2 * cf, ch), BF),
        in_specs=[
            pl.BlockSpec((rf + 2, cf + 2, SUB, ch), lambda r: (0, 0, 0, 0)),
            pl.BlockSpec(spread.shape, lambda r: (0, 0)),
            pl.BlockSpec((1, ch), lambda r: (0, 0)),
        ],
        out_specs=pl.BlockSpec((batch, groups, 2, 2 * cf, ch), lambda r: (0, 0, r, 0, 0)),
    )(z, spread, fo.reshape(1, ch))
    return decoded.reshape(batch, 2 * hf, 2 * cf, ch)


def solution(mesh):
    image = P(None, "row", "col", None)
    return jax.shard_map(
        per_device,
        mesh=mesh,
        in_specs=(image, image, image) + (P(),) * 8,
        out_specs=image,
        check_vma=False,
    )
```
